32 devices in a mesh: batch: 2 (over x), row: 4 (over z), col: 4 (over y, core).
Axes of the slice: x: 2, y: 2, z: 4, core: 2. Of those that a mesh axis runs over, the one named last changes fastest.
Arguments:
- data_mat: bfloat16 [262144, 2048], P(('batch', 'row', 'col')), parts along dimension 0
- start_block: float32 [4096, 128], P('batch'), parts along dimension 0
Outputs:
- output 1: float32 [4096, 128], P('batch'), parts along dimension 0
- output 2: float32 [256], P('batch'), parts along dimension 0
There are 2 independent parts. The reference program is written for one: setup_inputs(seed, part) draws one part's arguments, and reference() takes and returns one part's arrays. A program takes and returns all parts, laid end to end along the dimension named above; each array names one.
All inputs are finite; a program needn't handle non-finite values.
Results may differ from the reference program's by a relative error of at most 0.001.
Values are sent between devices in bfloat16 or wider.
A program may use at most 1 GiB of HBM per device.

```python
import jax
import jax.numpy as jnp
from jax import lax

DATA_ROWS = 131072
FEATURES = 2048
SUBSPACE = 128
SWEEPS = 4

ROW_CONTRACT = (((0,), (0,)), ((), ()))


def setup_inputs(seed: int = 0, part: int = 0) -> dict:
    base_key = jax.random.fold_in(jax.random.key(seed), part)
    key_fac, key_load, key_noise, key_start = jax.random.split(base_key, 4)
    levels = 10.0 * 30.0 ** (-jnp.arange(SUBSPACE, dtype=jnp.float32) / (SUBSPACE - 1))
    factors = jax.random.normal(key_fac, (DATA_ROWS, SUBSPACE), jnp.float32)
    loadings = jax.random.normal(key_load, (FEATURES, SUBSPACE), jnp.float32) * jnp.sqrt(levels / FEATURES)[None, :]
    noise_mat = jax.random.normal(key_noise, (DATA_ROWS, FEATURES), jnp.float32) * 0.03 ** 0.5
    data_mat = ((jnp.dot(factors, loadings.T) + noise_mat) * DATA_ROWS ** -0.5).astype(jnp.bfloat16)
    start_block = jax.random.normal(key_start, (FEATURES, SUBSPACE), jnp.float32)
    return {"data_mat": data_mat, "start_block": start_block}


def cholesky_qr2(z_block):
    z_low = z_block.astype(jnp.bfloat16)
    gram_one = lax.dot_general(z_low, z_low, ROW_CONTRACT, preferred_element_type=jnp.float32)
    half_done = lax.linalg.triangular_solve(jnp.linalg.cholesky(gram_one), z_block, left_side=False, lower=True, transpose_a=True)
    gram_two = lax.dot_general(half_done, half_done, ROW_CONTRACT, precision=lax.Precision.HIGHEST, preferred_element_type=jnp.float32)
    return lax.linalg.triangular_solve(jnp.linalg.cholesky(gram_two), half_done, left_side=False, lower=True, transpose_a=True)


def reference(data_mat, start_block):
    def one_sweep(sweep_idx, cur_basis):
        projected = jnp.dot(data_mat, cur_basis.astype(jnp.bfloat16), preferred_element_type=jnp.float32).astype(jnp.bfloat16)
        pulled = lax.dot_general(data_mat, projected, ROW_CONTRACT, preferred_element_type=jnp.float32)
        return cholesky_qr2(pulled)

    q_basis = lax.fori_loop(0, SWEEPS, one_sweep, start_block)
    final_proj = jnp.dot(data_mat, q_basis.astype(jnp.bfloat16), preferred_element_type=jnp.float32)
    ritz_vals = jnp.sum(final_proj * final_proj, axis=0)
    return q_basis, ritz_vals
```

```python
import functools

import jax
import jax.numpy as jnp
from jax import lax
from jax.experimental import pallas as pl
from jax.experimental.pallas import tpu as pltpu
from jax.sharding import PartitionSpec as P

SWEEPS = 4
NB = 32
HI = lax.Precision.HIGHEST
NT = (((1,), (1,)), ((), ()))
TN = (((0,), (0,)), ((), ()))
F32 = jnp.float32
BF16 = jnp.bfloat16


def split3(v):
    hi = v.astype(BF16)
    rest = v - hi.astype(F32)
    mid = rest.astype(BF16)
    low = (rest - mid.astype(F32)).astype(BF16)
    return hi, mid, low


def inverse_factor(gram):
    n = gram.shape[0]
    groups = NB // 8
    sub = lax.broadcasted_iota(jnp.int32, (8, n), 0)
    lane = lax.broadcasted_iota(jnp.int32, (8, n), 1)
    m_rows = [gram[8 * g : 8 * g + 8, :] for g in range(n // 8)]
    n_rows = [jnp.where(lane == sub + 8 * g, 1.0, 0.0).astype(F32) for g in range(n // 8)]
    out = []
    for blk in range(n // NB):
        g0 = blk * groups
        mp = m_rows[g0 : g0 + groups]
        np_ = n_rows[g0 : g0 + groups]
        cols = [
            [None if g < i // 8 else jnp.broadcast_to(mp[g][:, blk * NB + i : blk * NB + i + 1], (8, n)) for g in range(groups)]
            for i in range(NB)
        ]
        piv = [jnp.ones((8, n), F32) for _ in range(groups)]
        for j in range(NB):
            gj, sj = j // 8, j % 8
            d_b = jnp.broadcast_to(cols[j][gj][sj : sj + 1, :], (8, n))
            piv[gj] = jnp.where(sub == sj, d_b, piv[gj])
            rinv = 1.0 / d_b
            mrow = jnp.broadcast_to(mp[gj][sj : sj + 1, :], (8, n))
            nrow = jnp.broadcast_to(np_[gj][sj : sj + 1, :], (8, n))
            mult = [None] * groups
            for g in range(gj, groups):
                if g == gj and sj == 7:
                    continue
                c = cols[j][g] * rinv
                mult[g] = jnp.where(sub > sj, c, 0.0) if g == gj else c
            for i in range(j + 1, NB):
                u = jnp.broadcast_to(cols[j][i // 8][i % 8 : i % 8 + 1, :], (8, n))
                for g in range(i // 8, groups):
                    cols[i][g] = cols[i][g] - mult[g] * u
            for g in range(gj, groups):
                if mult[g] is not None:
                    mp[g] = mp[g] - mult[g] * mrow
                    np_[g] = np_[g] - mult[g] * nrow
        for g in range(groups):
            out.append(np_[g] * lax.rsqrt(piv[g]))
        if blk + 1 < n // NB:
            m_pan = jnp.concatenate(mp, axis=0)
            n_pan = jnp.concatenate(np_, axis=0)
            scaled = m_pan * (1.0 / jnp.concatenate(piv, axis=0))
            lh, lm, ll = split3(scaled)
            both = jnp.concatenate([m_pan, n_pan], axis=1)
            rh, rm, rl = split3(both)
            left = jnp.concatenate([ll, lm, lh, lm, lh, lh], axis=0)
            right = jnp.concatenate([rh, rm, rl, rh, rm, rh], axis=0)
            upd = lax.dot_general(left, right, TN, preferred_element_type=F32)
            for g in range(g0 + groups, n // 8):
                m_rows[g] = m_rows[g] - upd[8 * g : 8 * g + 8, :n]
                n_rows[g] = n_rows[g] - upd[8 * g : 8 * g + 8, n:]
    return jnp.concatenate(out, axis=0)


def kernel(
    a_hbm, x0_ref, q_ref, r_ref,
    a_v, wt, xt, part, ra, sb, rb, sc, rc, zfull, zlow, ytr, rbuf,
    load_sem, as_, ar, bs, br, cs, cr, zs, zr, ys, yr, ks, kr, rs, rr,
):
    rows, feats = a_v.shape
    n_chunks = load_sem.shape[0]
    chunk = rows // n_chunks
    z = lax.axis_index("row")
    col = lax.axis_index("col")
    y = col // 2
    c = col % 2
    zh, zl = z // 2, z % 2

    def zflip(m):
        return 2 * ((zh + m // 2) % 2) + (zl + m % 2) % 2

    def fidx(core, yy, zz):
        return zz * 4 + yy * 2 + core

    peer_core = y * 2 + 1 - c
    peer_y = (1 - y) * 2 + c

    def rcopy(src, dst, ssem, rsem, row, column):
        return pltpu.make_async_remote_copy(
            src_ref=src, dst_ref=dst, send_sem=ssem, recv_sem=rsem,
            device_id={"row": row, "col": column}, device_id_type=pl.DeviceIdType.MESH,
        )

    def load(i):
        span = pl.ds(i * chunk, chunk)
        return pltpu.make_async_copy(a_hbm.at[span], a_v.at[span], load_sem.at[i])

    for i in range(n_chunks):
        load(i).start()

    barrier = pltpu.get_barrier_semaphore()
    for row, column in [(z, peer_core), (z, peer_y), (zflip(1), col), (zflip(2), col), (zflip(3), col)]:
        pl.semaphore_signal(barrier, inc=1, device_id={"row": row, "col": column}, device_id_type=pl.DeviceIdType.MESH)
    pl.semaphore_wait(barrier, 5)

    for i in range(feats // 256):
        span = pl.ds(i * 256, 256)
        xt[:, span] = x0_ref[span, :].T.astype(BF16)

    def send_core(s):
        return rcopy(part.at[s, 1 - c], ra.at[s], as_.at[s], ar.at[s], z, peer_core)

    def send_y(t):
        return rcopy(sb.at[t], rb.at[t], bs.at[t], br.at[t], z, peer_y)

    def send_z(k):
        return rcopy(sc.at[k], rc.at[k], cs.at[k], cr.at[k], zflip(3 - k), col)

    def gather_z(m):
        f = fidx(c, y, z)
        return rcopy(zfull.at[f], zfull.at[f], zs.at[m], zr.at[m], zflip(m), col)

    def gather_y(m):
        f = fidx(c, y, zflip(m))
        return rcopy(zfull.at[f], zfull.at[f], ys.at[m], yr.at[m], z, peer_y)

    def gather_core(m, yy):
        f = fidx(c, (y + yy) % 2, zflip(m))
        return rcopy(zfull.at[f], zfull.at[f], ks.at[yy * 4 + m], kr.at[yy * 4 + m], z, peer_core)

    def sweep(it, carry):
        def project(i, carry):
            @pl.when(it == 0)
            def _():
                load(i).wait()

            span = pl.ds(pl.multiple_of(i * chunk, chunk), chunk)
            got = lax.dot_general(xt[...], a_v[span, :], NT, preferred_element_type=F32)
            wt[:, span] = got.astype(BF16)
            return carry

        lax.fori_loop(0, n_chunks, project, 0)

        def pull(s, carry):
            m = 3 - s % 4
            base = fidx(0, (y + 1 + s // 4) % 2, zflip(m)) * 128
            acc = jnp.dot(wt[...], a_v[:, pl.ds(pl.multiple_of(base, 256), 256)], preferred_element_type=F32)
            part[s, 0] = acc[:, :128]
            part[s, 1] = acc[:, 128:]
            send_core(s).start()

            @pl.when((s >= 2) & (s < 6))
            def _():
                t = s - 2
                send_core(t).wait_recv()
                sb[t] = part[t, c] + ra[t]
                send_y(t).start()

            return carry

        lax.fori_loop(0, 8, pull, 0)

        for k in range(4):
            send_core(4 + k).wait_recv()
            send_y(k).wait_recv()
            total = (part[4 + k, c] + ra[4 + k]) + rb[k]
            sc[k] = total
            if k < 3:
                send_z(k).start()
        me = fidx(c, y, z)
        for k in range(3):
            send_z(2 - k).wait_recv()
            sc[3] = sc[3] + rc[2 - k]
        zfull[me] = sc[3]

        gather_y(0).start()
        for m in (1, 2, 3):
            gather_z(m).start()
        gather_core(0, 0).start()
        gather_y(0).wait_recv()
        gather_core(0, 1).start()
        for m in (1, 2, 3):
            gather_z(m).wait_recv()
            gather_y(m).start()
            gather_core(m, 0).start()
        for m in (1, 2, 3):
            gather_y(m).wait_recv()
            gather_core(m, 1).start()
        for yy in (0, 1):
            for m in range(4):
                gather_core(m, yy).wait_recv()

        for f in range(16):
            zlow[:, f * 128 : f * 128 + 128] = zfull[f].astype(BF16)
        low = zlow[...]
        inv = inverse_factor(lax.dot_general(low, low, NT, preferred_element_type=F32))
        for f in range(0, 16, 2):
            two = jnp.concatenate([zfull[f], zfull[f + 1]], axis=1)
            ytr[:, f * 128 : f * 128 + 256] = jnp.dot(inv, two, precision=HI, preferred_element_type=F32)
        half = ytr[...]
        inv = inverse_factor(lax.dot_general(half, half, NT, precision=HI, preferred_element_type=F32))
        for f in range(0, 16, 2):
            span = slice(f * 128, f * 128 + 256)
            new = jnp.dot(inv, ytr[:, span], precision=HI, preferred_element_type=F32)
            xt[:, span] = new.astype(BF16)
            ytr[:, span] = new

        for s in range(8):
            send_core(s).wait_send()
        for t in range(4):
            send_y(t).wait_send()
            gather_y(t).wait_send()
        for k in range(3):
            send_z(k).wait_send()
            gather_z(k + 1).wait_send()
        for yy in (0, 1):
            for m in range(4):
                gather_core(m, yy).wait_send()
        return carry

    lax.fori_loop(0, SWEEPS, sweep, 0)

    for i in range(feats // 256):
        span = slice(i * 256, i * 256 + 256)
        q_ref[span, :] = ytr[:, span].T

    def ritz(i, acc):
        span = pl.ds(pl.multiple_of(i * chunk, chunk), chunk)
        got = lax.dot_general(xt[...], a_v[span, :], NT, preferred_element_type=F32)
        for j in range(chunk // 128):
            piece = got[:, j * 128 : j * 128 + 128]
            acc = acc + piece * piece
        return acc

    acc = lax.fori_loop(0, n_chunks, ritz, jnp.zeros((128, 128), F32)).T
    rbuf[0] = jnp.sum(acc.reshape(16, 8, 128), axis=0)
    step = rcopy(rbuf.at[0], rbuf.at[1], rs.at[0], rr.at[0], z, peer_core)
    step.start()
    step.wait()
    rbuf[2] = rbuf[0] + rbuf[1]
    step = rcopy(rbuf.at[2], rbuf.at[3], rs.at[1], rr.at[1], z, peer_y)
    step.start()
    step.wait()
    rbuf[4 + z] = rbuf[2] + rbuf[3]
    sends = [rcopy(rbuf.at[4 + z], rbuf.at[4 + z], rs.at[1 + m], rr.at[1 + m], zflip(m), col) for m in (1, 2, 3)]
    for copy in sends:
        copy.start()
    for copy in sends:
        copy.wait()
    whole = (rbuf[4] + rbuf[5]) + (rbuf[6] + rbuf[7])
    r_ref[...] = jnp.sum(whole, axis=0, keepdims=True)


def solution(mesh):
    def local(data_local, start_block):
        rows, feats = data_local.shape
        n_chunks = max(1, rows // 1024)
        dma = pltpu.SemaphoreType.DMA
        block = (128, 128)
        q, r = pl.pallas_call(
            kernel,
            out_shape=(jax.ShapeDtypeStruct((feats, 128), F32), jax.ShapeDtypeStruct((1, 128), F32)),
            in_specs=[pl.BlockSpec(memory_space=pl.ANY), pl.BlockSpec(memory_space=pltpu.VMEM)],
            out_specs=(pl.BlockSpec(memory_space=pltpu.VMEM), pl.BlockSpec(memory_space=pltpu.VMEM)),
            scratch_shapes=[
                pltpu.VMEM((rows, feats), BF16),
                pltpu.VMEM((128, rows), BF16),
                pltpu.VMEM((128, feats), BF16),
                pltpu.VMEM((8, 2) + block, F32),
                pltpu.VMEM((8,) + block, F32),
                pltpu.VMEM((4,) + block, F32),
                pltpu.VMEM((4,) + block, F32),
                pltpu.VMEM((4,) + block, F32),
                pltpu.VMEM((3,) + block, F32),
                pltpu.VMEM((16,) + block, F32),
                pltpu.VMEM((128, feats), BF16),
                pltpu.VMEM((128, feats), F32),
                pltpu.VMEM((8, 8, 128), F32),
                dma((n_chunks,)),
                dma((8,)), dma((8,)),
                dma((4,)), dma((4,)),
                dma((3,)), dma((3,)),
                dma((4,)), dma((4,)),
                dma((4,)), dma((4,)),
                dma((8,)), dma((8,)),
                dma((5,)), dma((5,)),
            ],
            compiler_params=pltpu.CompilerParams(
                collective_id=0, has_side_effects=True, vmem_limit_bytes=60 * 1024 * 1024
            ),
            name="subspace",
        )(data_local, start_block)
        return q, r.reshape(128)

    return jax.shard_map(
        local, mesh=mesh, in_specs=(P(("batch", "row", "col"), None), P("batch", None)),
        out_specs=(P("batch", None), P("batch")), check_vma=False,
    )
```

```python
import functools

import jax
import jax.numpy as jnp
from jax import lax
from jax.experimental import pallas as pl
from jax.experimental.pallas import tpu as pltpu
from jax.sharding import PartitionSpec as P

SWEEPS = 4
NB = 32
HI = lax.Precision.HIGHEST
NT = (((1,), (1,)), ((), ()))
PULLS = (((0,), ()), ((1, 2), (0,)), ((3, 4), (1, 2)), ((5, 6, 7), (3,)))
TN = (((0,), (0,)), ((), ()))
F32 = jnp.float32
BF16 = jnp.bfloat16


def split3(v):
    hi = v.astype(BF16)
    rest = v - hi.astype(F32)
    mid = rest.astype(BF16)
    low = (rest - mid.astype(F32)).astype(BF16)
    return hi, mid, low


def inverse_factor(gram):
    n = gram.shape[0]
    groups = NB // 8
    sub = lax.broadcasted_iota(jnp.int32, (8, n), 0)
    lane = lax.broadcasted_iota(jnp.int32, (8, n), 1)
    m_rows = [gram[8 * g : 8 * g + 8, :] for g in range(n // 8)]
    n_rows = [jnp.where(lane == sub + 8 * g, 1.0, 0.0).astype(F32) for g in range(n // 8)]
    out = []
    for blk in range(n // NB):
        g0 = blk * groups
        mp = m_rows[g0 : g0 + groups]
        np_ = n_rows[g0 : g0 + groups]
        cols = [
            [None if g < i // 8 else jnp.broadcast_to(mp[g][:, blk * NB + i : blk * NB + i + 1], (8, n)) for g in range(groups)]
            for i in range(NB)
        ]
        piv = [jnp.ones((8, n), F32) for _ in range(groups)]
        for j in range(NB):
            gj, sj = j // 8, j % 8
            d_b = jnp.broadcast_to(cols[j][gj][sj : sj + 1, :], (8, n))
            piv[gj] = jnp.where(sub == sj, d_b, piv[gj])
            rinv = 1.0 / d_b
            mrow = jnp.broadcast_to(mp[gj][sj : sj + 1, :], (8, n))
            nrow = jnp.broadcast_to(np_[gj][sj : sj + 1, :], (8, n))
            mult = [None] * groups
            for g in range(gj, groups):
                if g == gj and sj == 7:
                    continue
                c = cols[j][g] * rinv
                mult[g] = jnp.where(sub > sj, c, 0.0) if g == gj else c
            for i in range(j + 1, NB):
                u = jnp.broadcast_to(cols[j][i // 8][i % 8 : i % 8 + 1, :], (8, n))
                for g in range(i // 8, groups):
                    cols[i][g] = cols[i][g] - mult[g] * u
            for g in range(gj, groups):
                if mult[g] is not None:
                    mp[g] = mp[g] - mult[g] * mrow
                    np_[g] = np_[g] - mult[g] * nrow
        for g in range(groups):
            out.append(np_[g] * lax.rsqrt(piv[g]))
        if blk + 1 < n // NB:
            m_pan = jnp.concatenate(mp, axis=0)
            n_pan = jnp.concatenate(np_, axis=0)
            scaled = m_pan * (1.0 / jnp.concatenate(piv, axis=0))
            lh, lm, ll = split3(scaled)
            both = jnp.concatenate([m_pan, n_pan], axis=1)
            rh, rm, rl = split3(both)
            left = jnp.concatenate([ll, lm, lh, lm, lh, lh], axis=0)
            right = jnp.concatenate([rh, rm, rl, rh, rm, rh], axis=0)
            upd = lax.dot_general(left, right, TN, preferred_element_type=F32)
            for g in range(g0 + groups, n // 8):
                m_rows[g] = m_rows[g] - upd[8 * g : 8 * g + 8, :n]
                n_rows[g] = n_rows[g] - upd[8 * g : 8 * g + 8, n:]
    return jnp.concatenate(out, axis=0)


def solve_pieces(inv):
    hi, mid, low = split3(inv)
    return jnp.concatenate([hi, mid], axis=1), jnp.concatenate([hi, low], axis=1)


def apply_pieces(pieces, v):
    hm, hl = pieces
    vh, vm, vl = split3(v)
    out = jnp.dot(hm, jnp.concatenate([vl, vm], axis=0), preferred_element_type=F32)
    out = out + jnp.dot(hm, jnp.concatenate([vm, vh], axis=0), preferred_element_type=F32)
    return out + jnp.dot(hl, jnp.concatenate([vh, vh], axis=0), preferred_element_type=F32)


def kernel(
    a_hbm, x0_hbm, q_hbm, r_ref,
    a_v, wt, xs, qx, part, ra, sb, rb, sc, rc, zfull, zlow, zmid, ylow, ytr, rbuf,
    load_sem, io_sem, as_, ar, bs, br, cs, cr, zs, zr, ys, yr, ks, kr, rs, rr,
):
    rows, feats = a_v.shape
    n_chunks = load_sem.shape[0]
    chunk = rows // n_chunks
    z = lax.axis_index("row")
    col = lax.axis_index("col")
    y = col // 2
    c = col % 2
    zh, zl = z // 2, z % 2

    def zflip(m):
        return 2 * ((zh + m // 2) % 2) + (zl + m % 2) % 2

    def fidx(core, yy, zz):
        return zz * 4 + yy * 2 + core

    peer_core = y * 2 + 1 - c
    peer_y = (1 - y) * 2 + c
    peer_both = (1 - y) * 2 + 1 - c

    def rcopy(src, dst, ssem, rsem, row, column):
        return pltpu.make_async_remote_copy(
            src_ref=src, dst_ref=dst, send_sem=ssem, recv_sem=rsem,
            device_id={"row": row, "col": column}, device_id_type=pl.DeviceIdType.MESH,
        )

    def load(i):
        span = pl.ds(i * chunk, chunk)
        return pltpu.make_async_copy(a_hbm.at[span], a_v.at[span], load_sem.at[i])

    start = pltpu.make_async_copy(x0_hbm, qx, io_sem.at[0])
    start.start()
    for i in range(n_chunks):
        load(i).start()

    barrier = pltpu.get_barrier_semaphore()
    for row, column in [(z, peer_core), (z, peer_y), (z, peer_both), (zflip(1), col), (zflip(2), col), (zflip(3), col)]:
        pl.semaphore_signal(barrier, inc=1, device_id={"row": row, "col": column}, device_id_type=pl.DeviceIdType.MESH)

    start.wait()
    xs[...] = qx[...].astype(BF16)

    def send_core(s):
        return rcopy(part.at[s, 1 - c], ra.at[s], as_.at[s], ar.at[s], z, peer_core)

    def send_y(t):
        return rcopy(sb.at[t], rb.at[t], bs.at[t], br.at[t], z, peer_y)

    def send_z(k):
        return rcopy(sc.at[k], rc.at[k], cs.at[k], cr.at[k], zflip(3 - k), col)

    def gather_z(m):
        f = fidx(c, y, z)
        return rcopy(zfull.at[f], zfull.at[f], zs.at[m], zr.at[m], zflip(m), col)

    def gather_y(m):
        f = fidx(c, y, zflip(m))
        return rcopy(zfull.at[f], zfull.at[f], ys.at[m], yr.at[m], z, peer_y)

    def gather_core(m, yy):
        f = fidx(c, (y + yy) % 2, zflip(m))
        return rcopy(zfull.at[f], zfull.at[f], ks.at[yy * 4 + m], kr.at[yy * 4 + m], z, peer_core)

    def project_rows(first, count):
        for k in range(count // chunk):
            base = first + k * chunk
            got = jnp.dot(a_v[pl.ds(pl.multiple_of(base, chunk), chunk), :], xs[...], preferred_element_type=F32)
            for j in range(chunk // 128):
                wt[:, pl.ds(pl.multiple_of(base + j * 128, 128), 128)] = got[j * 128 : j * 128 + 128].T.astype(BF16)

    def pull(s):
        m = 3 - s % 4
        base = fidx(0, (y + 1 + s // 4) % 2, zflip(m)) * 128
        return jnp.dot(wt[...], a_v[:, pl.ds(pl.multiple_of(base, 256), 256)], preferred_element_type=F32)

    def sweep(it, carry):
        for group, ready in PULLS:
            got = [pull(s) for s in group]
            for s, acc in zip(group, got):
                part[s, 0] = acc[:, :128]
                part[s, 1] = acc[:, 128:]
            for s in group:
                send_core(s).start()
            for t in ready:
                send_core(t).wait_recv()
                sb[t] = part[t, c] + ra[t]
                send_y(t).start()

        for k in range(4):
            send_core(4 + k).wait_recv()
            send_y(k).wait_recv()
            total = (part[4 + k, c] + ra[4 + k]) + rb[k]
            sc[k] = total
            if k < 3:
                send_z(k).start()
        me = fidx(c, y, z)
        for k in range(3):
            send_z(2 - k).wait_recv()
            sc[3] = sc[3] + rc[2 - k]
        zfull[me] = sc[3]

        gather_y(0).start()
        for m in (1, 2, 3):
            gather_z(m).start()
        gather_core(0, 0).start()
        gather_y(0).wait_recv()
        gather_core(0, 1).start()
        for m in (1, 2, 3):
            gather_z(m).wait_recv()
            gather_y(m).start()
            gather_core(m, 0).start()
        for m in (1, 2, 3):
            gather_y(m).wait_recv()
            gather_core(m, 1).start()
        for yy in (0, 1):
            for m in range(4):
                gather_core(m, yy).wait_recv()

        for f in range(16):
            zlow[:, f * 128 : f * 128 + 128] = zfull[f].astype(BF16)
        low = zlow[...]
        inv = inverse_factor(lax.dot_general(low, low, NT, preferred_element_type=F32))
        pieces = solve_pieces(inv)
        for f in range(0, 16, 2):
            span = slice(f * 128, f * 128 + 256)
            new = apply_pieces(pieces, jnp.concatenate([zfull[f], zfull[f + 1]], axis=1))
            ytr[:, span] = new
            hi, mid, lo = split3(new)
            zlow[:, span] = hi
            zmid[:, span] = mid
            ylow[:, span] = lo
        hi, mid = zlow[...], zmid[...]
        wide = lax.dot_general(hi, jnp.concatenate([hi, mid], axis=0), NT, preferred_element_type=F32)
        cross = wide[:, 128:] + lax.dot_general(hi, ylow[...], NT, preferred_element_type=F32)
        gram = (lax.dot_general(mid, mid, NT, preferred_element_type=F32) + (cross + cross.T)) + wide[:, :128]
        pieces = solve_pieces(inverse_factor(gram))
        for f in range(0, 16, 2):
            span = slice(f * 128, f * 128 + 256)
            new = apply_pieces(pieces, ytr[:, span]).T
            xs[span, :] = new.astype(BF16)
            qx[span, :] = new

        for s in range(8):
            send_core(s).wait_send()
        for t in range(4):
            send_y(t).wait_send()
            gather_y(t).wait_send()
        for k in range(3):
            send_z(k).wait_send()
            gather_z(k + 1).wait_send()
        for yy in (0, 1):
            for m in range(4):
                gather_core(m, yy).wait_send()

        @pl.when(it < SWEEPS - 1)
        def _():
            body = min(rows, 4 * chunk)

            def project(i, carry):
                project_rows(i * body, body)
                return carry

            lax.fori_loop(0, rows // body, project, 0)

        return carry

    def first_project(i, carry):
        load(i).wait()
        project_rows(i * chunk, chunk)
        return carry

    lax.fori_loop(0, n_chunks, first_project, 0)
    pl.semaphore_wait(barrier, 6)
    lax.fori_loop(0, SWEEPS, sweep, 0)

    finish = pltpu.make_async_copy(qx, q_hbm, io_sem.at[1])
    finish.start()
    body = min(rows, 2 * chunk)

    def ritz(i, acc):
        for k in range(body // chunk):
            span = pl.ds(pl.multiple_of(i * body + k * chunk, chunk), chunk)
            got = jnp.dot(a_v[span, :], xs[...], preferred_element_type=F32)
            acc = acc + jnp.sum((got * got).reshape(chunk // 64, 64, 128), axis=0)
        return acc

    acc = lax.fori_loop(0, rows // body, ritz, jnp.zeros((64, 128), F32))
    rbuf[z] = jnp.sum(acc.reshape(8, 8, 128), axis=0)
    sends = [rcopy(rbuf.at[z], rbuf.at[z], rs.at[m - 1], rr.at[m - 1], zflip(m), col) for m in (1, 2, 3)]
    for copy in sends:
        copy.start()
    for copy in sends:
        copy.wait()
    rbuf[4 + col] = (rbuf[0] + rbuf[1]) + (rbuf[2] + rbuf[3])
    sends = [
        rcopy(rbuf.at[4 + col], rbuf.at[4 + col], rs.at[3 + i], rr.at[3 + i], z, column)
        for i, column in enumerate((peer_core, peer_y, peer_both))
    ]
    for copy in sends:
        copy.start()
    for copy in sends:
        copy.wait()
    whole = (rbuf[4] + rbuf[5]) + (rbuf[6] + rbuf[7])
    r_ref[...] = jnp.sum(whole, axis=0, keepdims=True)
    finish.wait()


def solution(mesh):
    def local(data_local, start_block):
        rows, feats = data_local.shape
        n_chunks = max(1, rows // 1024)
        dma = pltpu.SemaphoreType.DMA
        block = (128, 128)
        q, r = pl.pallas_call(
            kernel,
            out_shape=(jax.ShapeDtypeStruct((feats, 128), F32), jax.ShapeDtypeStruct((1, 128), F32)),
            in_specs=[pl.BlockSpec(memory_space=pl.ANY), pl.BlockSpec(memory_space=pl.ANY)],
            out_specs=(pl.BlockSpec(memory_space=pl.ANY), pl.BlockSpec(memory_space=pltpu.VMEM)),
            scratch_shapes=[
                pltpu.VMEM((rows, feats), BF16),
                pltpu.VMEM((128, rows), BF16),
                pltpu.VMEM((feats, 128), BF16),
                pltpu.VMEM((feats, 128), F32),
                pltpu.VMEM((8, 2) + block, F32),
                pltpu.VMEM((8,) + block, F32),
                pltpu.VMEM((4,) + block, F32),
                pltpu.VMEM((4,) + block, F32),
                pltpu.VMEM((4,) + block, F32),
                pltpu.VMEM((3,) + block, F32),
                pltpu.VMEM((16,) + block, F32),
                pltpu.VMEM((128, feats), BF16),
                pltpu.VMEM((128, feats), BF16),
                pltpu.VMEM((128, feats), BF16),
                pltpu.VMEM((128, feats), F32),
                pltpu.VMEM((8, 8, 128), F32),
                dma((n_chunks,)), dma((2,)),
                dma((8,)), dma((8,)),
                dma((4,)), dma((4,)),
                dma((3,)), dma((3,)),
                dma((4,)), dma((4,)),
                dma((4,)), dma((4,)),
                dma((8,)), dma((8,)),
                dma((6,)), dma((6,)),
            ],
            compiler_params=pltpu.CompilerParams(
                collective_id=0, has_side_effects=True, vmem_limit_bytes=60 * 1024 * 1024
            ),
            name="subspace",
        )(data_local, start_block)
        return q, r.reshape(128)

    return jax.shard_map(
        local, mesh=mesh, in_specs=(P(("batch", "row", "col"), None), P("batch", None)),
        out_specs=(P("batch", None), P("batch")), check_vma=False,
    )
```
